32 devices in a mesh: seq: 16 (over z, y, core), head: 2 (over x).
Axes of the slice: x: 2, y: 2, z: 4, core: 2. Of those that a mesh axis runs over, the one named last changes fastest.
Arguments:
- sequence: bfloat16 [8192, 2048], P('seq'), may hold values from -6 to 6
- input_weight: bfloat16 [2048, 4096], P(None, 'head'), may hold values from -0.125 to 0.125
- gate_weight: bfloat16 [2048, 4096], P(None, 'head'), may hold values from -0.125 to 0.125
- state_weight: bfloat16 [2048, 256], replicated, may hold values from -0.015625 to 0.015625
- step_weight: bfloat16 [2048, 64], P(None, 'head'), may hold values from -0.125 to 0.125
- step_bias: float32 [64], P('head'), may hold values from -2 to 0
- decay_rate: float32 [64], P('head'), may hold values from 6.1035156e-05 to 0.1
- skip_gain: float32 [64], P('head'), may hold values from 0.5 to 1.5
- output_weight: bfloat16 [4096, 2048], P('head'), may hold values from -0.09375 to 0.09375
Outputs:
- encoded: bfloat16 [8192, 2048], P('seq', 'head')
The draws below stay inside these ranges and needn't reach their ends.
All inputs are finite; a program needn't handle non-finite values.
Results may differ from the reference program's by a relative error of at most 0.014.
Values sent between devices are 32-bit elements; how exact they have to be, the bound alone decides.
A program may use at most 128 MiB of HBM per device.

```python
import math
import jax
import jax.numpy as jnp
from jax import lax

D = 2048
HEADS = 64
HEADDIM = 64
STATE = 128
SEQ_DEV = 512
LENGTH = 8192


def steps_of(key, dims, cuts, least, high):
    loudness = 1.0
    for dim, parts in cuts:
        heights = jax.random.uniform(jax.random.fold_in(jax.random.fold_in(key, 6), dim), (parts,), jnp.float32, least / len(cuts), high / len(cuts))
        loudness = loudness * jnp.repeat(jnp.exp(heights), dims[dim] // parts).reshape((-1,) + (1,) * (len(dims) - 1 - dim))
    return loudness


def bell_draw(stream_key, extent, scale, most, shards=(), kind=jnp.bfloat16):
    gain = steps_of(stream_key, extent, shards, -0.22, 0.18) if shards else 1.0
    array = jax.random.normal(stream_key, extent, jnp.float32) * scale * gain
    return jnp.minimum(jnp.maximum(array, -most), most).astype(kind)


def setup_inputs(seed: int = 0) -> dict:
    splits = jax.random.split(jax.random.key(seed), 10)
    return {
        "sequence": bell_draw(splits[0], (LENGTH, D), 1.0, 6.0, ((0, 16),)),
        "input_weight": bell_draw(splits[1], (D, HEADS * HEADDIM), D ** -0.5, 0.125, ((1, 2),)),
        "gate_weight": bell_draw(splits[2], (D, HEADS * HEADDIM), D ** -0.5, 0.125, ((1, 2),)),
        "state_weight": bell_draw(splits[3], (D, 2 * STATE), (D * 64) ** -0.5, 0.015625),
        "step_weight": bell_draw(splits[4], (D, HEADS), D ** -0.5, 0.125, ((1, 2),)),
        "step_bias": jnp.clip(-2.0 + 2.0 * jax.random.uniform(splits[5], (HEADS,), jnp.float32) ** steps_of(splits[5], (HEADS,), ((0, 2),), -0.2, 0.2), -2.0, 0.0),
        "decay_rate": jnp.clip(jnp.exp(math.log(0.1) - 7.4014754 * jax.random.uniform(splits[6], (HEADS,), jnp.float32) ** steps_of(splits[6], (HEADS,), ((0, 2),), -0.2, 0.2)), 6.103515625e-05, 0.1),
        "skip_gain": jnp.clip(0.5 + 1.0 * jax.random.uniform(splits[7], (HEADS,), jnp.float32) ** steps_of(splits[7], (HEADS,), ((0, 2),), -0.2, 0.2), 0.5, 1.5),
        "output_weight": bell_draw(splits[8], (HEADS * HEADDIM, D), (HEADS * HEADDIM) ** -0.5, 0.09375, ((0, 2),)),
    }


def project(sequence, input_weight, gate_weight, state_weight, step_weight, step_bias):
    inputs = jnp.dot(sequence, input_weight, preferred_element_type=jnp.float32).astype(jnp.bfloat16)
    gates = jnp.dot(sequence, gate_weight, preferred_element_type=jnp.float32).astype(jnp.bfloat16)
    state_proj = jnp.dot(sequence, state_weight, preferred_element_type=jnp.float32).astype(jnp.bfloat16)
    raw_steps = jnp.dot(sequence, step_weight, preferred_element_type=jnp.float32) + step_bias[None, :]
    step_sizes = jax.nn.softplus(raw_steps).astype(jnp.bfloat16)
    return inputs, gates, state_proj, step_sizes


def group_parts(inputs, state_proj, step_sizes, decay_rate):
    row_count, head_count = step_sizes.shape
    state_size = state_proj.shape[1] // 2
    per_head = inputs.reshape(row_count, head_count, -1)
    writer = state_proj[:, :state_size]
    reader = state_proj[:, state_size:]
    step_float = step_sizes.astype(jnp.float32)
    log_decay = jnp.cumsum(-decay_rate[None, :] * step_float, axis=0)
    by_head = log_decay.T
    affinity = jnp.dot(reader, writer.T, preferred_element_type=jnp.float32)
    causal = lax.broadcasted_iota(jnp.int32, (row_count, row_count), 0) >= lax.broadcasted_iota(jnp.int32, (row_count, row_count), 1)
    spread = jnp.where(causal[None], by_head[:, :, None] - by_head[:, None, :], jnp.float32(0.0))
    decays = jnp.where(causal[None], jnp.exp(spread), jnp.float32(0.0))
    mixing = (affinity[None] * decays * step_float.T[:, None, :]).astype(jnp.bfloat16)
    inside = jnp.einsum("hts,shp->thp", mixing.astype(jnp.float32), per_head.astype(jnp.float32))
    to_end = jnp.exp(log_decay[-1][None, :] - log_decay) * step_float
    weighted = (per_head.astype(jnp.float32) * to_end[:, :, None]).astype(jnp.bfloat16)
    local_state = jnp.einsum("shp,sn->hpn", weighted.astype(jnp.float32), writer.astype(jnp.float32))
    totals = jnp.exp(log_decay[-1])
    return inside, log_decay, totals, local_state


def finish(inside, log_decay, carry_in, state_proj, inputs, gates, skip_gain):
    row_count, head_count = log_decay.shape
    state_size = state_proj.shape[1] // 2
    reader = state_proj[:, state_size:].astype(jnp.float32)
    per_head = inputs.reshape(row_count, head_count, -1).astype(jnp.float32)
    carried = jnp.einsum("tn,hpn->thp", reader, carry_in, precision=lax.Precision.HIGHEST)
    result = inside + jnp.exp(log_decay)[:, :, None] * carried + skip_gain[None, :, None] * per_head
    result = result.reshape(row_count, -1)
    return (result * jax.nn.silu(gates.astype(jnp.float32))).astype(jnp.bfloat16)


def branch(sequence, input_weight, gate_weight, state_weight, step_weight, step_bias, decay_rate, skip_gain):
    inputs, gates, state_proj, step_sizes = project(sequence, input_weight, gate_weight, state_weight, step_weight, step_bias)
    group_count = sequence.shape[0] // SEQ_DEV

    def advance(carry_in, pieces):
        part_in, part_gate, part_state, part_step = pieces
        inside, log_decay, totals, local_state = group_parts(part_in, part_state, part_step, decay_rate)
        out_rows = finish(inside, log_decay, carry_in, part_state, part_in, part_gate, skip_gain)
        return totals[:, None, None] * carry_in + local_state, out_rows

    pieces = (inputs.reshape(group_count, SEQ_DEV, inputs.shape[1]),
              gates.reshape(group_count, SEQ_DEV, gates.shape[1]),
              state_proj.reshape(group_count, SEQ_DEV, state_proj.shape[1]),
              step_sizes.reshape(group_count, SEQ_DEV, step_sizes.shape[1]))
    start = jnp.zeros((HEADS, HEADDIM, STATE), jnp.float32)
    final_state, rows_out = lax.scan(advance, start, pieces)
    return rows_out.reshape(sequence.shape[0], -1)


def reference(sequence, input_weight, gate_weight, state_weight, step_weight, step_bias, decay_rate, skip_gain, output_weight):
    forward = branch(sequence, input_weight, gate_weight, state_weight, step_weight, step_bias, decay_rate, skip_gain)
    mirrored = sequence[::-1, ::-1]
    backward_mirror = branch(mirrored, input_weight, gate_weight, state_weight, step_weight, step_bias, decay_rate, skip_gain)
    backward = backward_mirror[::-1]
    summed = jnp.dot(forward, output_weight, preferred_element_type=jnp.float32)
    summed = summed + jnp.dot(backward, output_weight[:, ::-1], preferred_element_type=jnp.float32)
    return summed.astype(jnp.bfloat16)
```

```python
import functools

import jax
import jax.numpy as jnp
from jax import lax
from jax.experimental import pallas as pl
from jax.experimental.pallas import tpu as pltpu
from jax.sharding import PartitionSpec as P

F32 = jnp.float32
BF16 = jnp.bfloat16
HEADDIM = 64
CHUNK = 128
LANES = 128
BLOCK = 256
STEP = 8


def eye_flip(size):
    r = lax.broadcasted_iota(jnp.int32, (size, size), 0)
    c = lax.broadcasted_iota(jnp.int32, (size, size), 1)
    return jnp.where(r + c == size - 1, 1.0, 0.0).astype(BF16)


def dot(a, b):
    return jnp.dot(a, b, preferred_element_type=F32)


def dot_first(a, b):
    return lax.dot_general(a, b, (((0,), (0,)), ((), ())), preferred_element_type=F32)


def dot_last(a, b):
    return lax.dot_general(a, b, (((1,), (1,)), ((), ())), preferred_element_type=F32)


def split(a):
    hi = a.astype(BF16)
    rest = a - hi.astype(F32)
    mid = rest.astype(BF16)
    low = (rest - mid.astype(F32)).astype(BF16)
    return hi, mid, low


def split_lanes(a, heads):
    hi, mid, low = split(a)
    lane = lax.broadcasted_iota(jnp.int32, a.shape, 1)
    low = jnp.where(lane < 3 * heads, low.astype(F32), 0.0)
    return jnp.where(
        lane < heads, hi.astype(F32), jnp.where(lane < 2 * heads, mid.astype(F32), low)
    ).astype(BF16)


def repeat_of(heads):
    r = lax.broadcasted_iota(jnp.int32, (heads, LANES), 0)
    c = lax.broadcasted_iota(jnp.int32, (heads, LANES), 1)
    hit = (c == r) | (c == r + heads) | (c == r + 2 * heads)
    return jnp.where(hit, 1.0, 0.0).astype(BF16)


def spread_of(heads, first, cols):
    r = lax.broadcasted_iota(jnp.int32, (LANES, cols), 0)
    c = lax.broadcasted_iota(jnp.int32, (LANES, cols), 1)
    head = lax.shift_right_logical(c, 6) + first
    hit = (r == head) | (r == head + heads) | (r == head + 2 * heads)
    return jnp.where(hit, 1.0, 0.0).astype(BF16)


def layer_kernel(
    plan,
    x_ref, stw_ref, sw_ref, bias_ref, rate_ref, gain_ref, inw_ref, gw_ref, ow_ref,
    out_ref,
    xf, proj, ldg, ldt, dtt, fac3, sin3, end3, spread, aff, skipw, logs, coef,
    wbuf, obuf, inp, gates, gated,
    ups, gots, chin, chout, ents, outs, sbuf, rbuf,
    w_sem, o_sem, lg_send, lg_recv, up_send, up_recv, ch_send, ch_recv, dn_send, dn_recv,
    x_send, x_recv,
):
    (groups, cols, levels, top, unit, n, peers, heads, per, total) = plan
    rows, depth = x_ref.shape
    state = stw_ref.shape[1] // 2
    hg = cols // HEADDIM
    tiles = cols // LANES
    count = rows // CHUNK
    me = lax.axis_index("seq")
    side = lax.axis_index("head")
    pos = me // unit
    bits = [(me // (1 << l)) % 2 for l in range(levels)]

    def mate(j):
        at = me
        for l in range(levels):
            if (j >> l) & 1:
                at = at + (1 << l) * (1 - 2 * bits[l])
        return at

    def ring(step):
        return me + (lax.rem(pos + step + top, top) - pos) * unit

    def w_copy(src, g):
        return pltpu.make_async_copy(
            src.at[:, pl.ds(pl.multiple_of(g * cols, LANES), cols)], wbuf.at[g], w_sem.at[g]
        )

    def o_copy(b):
        return pltpu.make_async_copy(
            ow_ref.at[:, pl.ds(b * BLOCK, BLOCK)], obuf.at[b], o_sem.at[b]
        )

    for g in range(groups):
        w_copy(inw_ref, g).start()

    barrier = pltpu.get_barrier_semaphore()
    greet = [mate(j) for j in range(1, 1 << levels)] + [ring(1), ring(-1)]
    for who in greet:
        pl.semaphore_signal(barrier, inc=1, device_id={"seq": who})
    for s in range(1, peers):
        pl.semaphore_signal(barrier, inc=1, device_id={"head": lax.rem(side + s, peers)})
    for d in (0, 1):
        @pl.when((pos if d == 0 else top - 1 - pos) == 0)
        def _():
            chin[:, d] = jnp.zeros_like(chin[:, d])
    pl.semaphore_wait(barrier, len(greet) + peers - 1)

    flip = eye_flip(BLOCK)
    blocks = depth // BLOCK
    for b in range(blocks):
        xf[:, b * BLOCK : (b + 1) * BLOCK] = dot(
            x_ref[:, (blocks - 1 - b) * BLOCK : (blocks - b) * BLOCK], flip
        ).astype(BF16)
    rep = repeat_of(heads)
    for g in range(groups):
        spread[g] = spread_of(heads, g * hg, cols)
    sw3 = dot(sw_ref[...], rep).astype(BF16)

    def tripled(ref):
        wide = jnp.broadcast_to(ref[...], (8, heads))
        a, b, c = split(wide)
        return dot(a, rep) + dot(b, rep) + dot(c, rep)

    bias = tripled(bias_ref)[0:1]
    rate = tripled(rate_ref)[0:1]
    gain = split_lanes(tripled(gain_ref), heads)
    for g in range(groups):
        skipw[g] = dot(gain, spread[g])
    r = lax.broadcasted_iota(jnp.int32, (rows, rows), 0)
    c = lax.broadcasted_iota(jnp.int32, (rows, rows), 1)
    for d in (0, 1):
        src = x_ref if d == 0 else xf
        raw = dot(src[...], sw3) + bias
        soft = jnp.maximum(raw, 0.0) + jnp.log1p(jnp.exp(-jnp.abs(raw)))
        steps = soft.astype(BF16).astype(F32)
        proj[d] = dot(src[...], stw_ref[...]).astype(BF16)
        tri = jnp.where((r >= c) if d == 0 else (r <= c), 1.0, 0.0).astype(BF16)
        va, vb, vc = split(-rate * steps)
        ld = dot(tri, va) + dot(tri, vb) + dot(tri, vc)
        end = ld[rows - 1 : rows] if d == 0 else ld[0:1]
        fac3[d] = split_lanes(jnp.exp(end - ld) * steps, heads)
        for k in range(count):
            at = slice(k * CHUNK, (k + 1) * CHUNK)
            ldk = ld[at]
            if d == 0:
                edge = ld[(k + 1) * CHUNK - 1 : (k + 1) * CHUNK]
                prev = ld[k * CHUNK - 1 : k * CHUNK] if k else None
            else:
                edge = ld[k * CHUNK : k * CHUNK + 1]
                prev = ld[(k + 1) * CHUNK : (k + 1) * CHUNK + 1] if k < count - 1 else None
            sin3[d, at] = split_lanes(jnp.exp(ldk if prev is None else ldk - prev), heads)
            end3[d, at] = split_lanes(jnp.exp(edge - ldk) * steps[at], heads)
            aff[d, k] = dot_last(proj[d, at, state:], proj[d, at, :state])
        flat_ld = ld.T
        flat_dt = steps.T
        ends = split_lanes(jnp.broadcast_to(end, (8, LANES)), heads)
        for g in range(groups):
            ldg[d, g] = pltpu.roll(ld, LANES - g * hg, axis=1) if g else ld
            ldt[d, g] = flat_ld[g * hg : (g + 1) * hg]
            dtt[d, g] = flat_dt[g * hg : (g + 1) * hg]
            wide = dot(ends, spread[g])
            for j in range(tiles):
                logs[0, d, g, j : j + 1] = wide[0:1, j * LANES : (j + 1) * LANES]

    def log_copy(j):
        return pltpu.make_async_remote_copy(
            src_ref=logs.at[0], dst_ref=logs.at[j], send_sem=lg_send.at[j],
            recv_sem=lg_recv.at[j], device_id={"seq": mate(j)},
        )

    def half_of(l):
        return state >> (l + 1)

    def rows_at(l, flag):
        return pl.ds(pl.multiple_of(flag * half_of(l), 8), half_of(l))

    def up_copy(l, g):
        return pltpu.make_async_remote_copy(
            src_ref=ups[l].at[g, :, rows_at(l, 1 - bits[l]), :], dst_ref=gots[l].at[g],
            send_sem=up_send.at[l, g], recv_sem=up_recv.at[l, g],
            device_id={"seq": mate(1 << l)},
        )

    def chain_copy(d, g):
        return pltpu.make_async_remote_copy(
            src_ref=chout.at[g, d], dst_ref=chin.at[g, d], send_sem=ch_send.at[d, g],
            recv_sem=ch_recv.at[d, g], device_id={"seq": ring(1 if d == 0 else -1)},
        )

    def down_copy(l, g):
        return pltpu.make_async_remote_copy(
            src_ref=outs[l].at[g], dst_ref=ents[l].at[g, :, rows_at(l, bits[l]), :],
            send_sem=dn_send.at[l, g], recv_sem=dn_recv.at[l, g],
            device_id={"seq": mate(1 << l)},
        )

    def late(l, d):
        flag = bits[l] if d == 0 else 1 - bits[l]
        return flag.astype(F32)

    def own_coef(l, d, g):
        return coef[2 * l, d, g]

    def other_coef(l, d, g):
        return coef[2 * l + 1, d, g]

    def combine(l, g):
        mine = rows_at(l, bits[l])
        for d in (0, 1):
            f = late(l, d)
            ea = f + (1.0 - f) * other_coef(l, d, g)
            eb = (1.0 - f) + f * own_coef(l, d, g)
            for j in range(tiles):
                at = slice(j * LANES, (j + 1) * LANES)
                ups[l + 1][g, d, :, at] = (
                    ea[j : j + 1] * ups[l][g, d, mine, at] + eb[j : j + 1] * gots[l][g, d, :, at]
                )

    def scatter_down(l, g):
        mine = rows_at(l, bits[l])
        for d in (0, 1):
            f = late(l, d)
            keep = f * other_coef(l, d, g) + (1.0 - f)
            give = f + (1.0 - f) * own_coef(l, d, g)
            for j in range(tiles):
                at = slice(j * LANES, (j + 1) * LANES)
                enter = chin[g, d, :, at] if l == levels - 1 else ents[l + 1][g, d, :, at]
                outs[l][g, d, :, at] = (
                    give[j : j + 1] * enter + (1.0 - f) * ups[l][g, d, mine, at]
                )
                ents[l][g, d, mine, at] = keep[j : j + 1] * enter + f * gots[l][g, d, :, at]

    def order(d):
        return pos if d == 0 else top - 1 - pos

    def hop(h, g, ok):
        for d in (0, 1):
            @pl.when(ok & (order(d) == h))
            def _():
                if h:
                    chain_copy(d, g).wait_recv()
                whole = coef[2 * levels, d, g]
                for j in range(tiles):
                    at = slice(j * LANES, (j + 1) * LANES)
                    chout[g, d, :, at] = (
                        whole[j : j + 1] * chin[g, d, :, at] + ups[levels][g, d, :, at]
                    )
                chain_copy(d, g).start()

    for j in range(1, 1 << levels):
        log_copy(j).start()

    def states(g):
        w_copy(inw_ref, g).wait()
        for d in (0, 1):
            src = x_ref if d == 0 else xf
            x = dot(src[...], wbuf[g]).astype(BF16)
            inp[g, d] = x
            wide = dot(fac3[d], spread[g])
            weighted = (inp[g, d].astype(F32) * wide).astype(BF16)
            ups[0][g, d] = dot_first(proj[d, :, :state], weighted)

    def gate(g):
        w_copy(gw_ref, g).wait()
        for d in (0, 1):
            src = x_ref if d == 0 else xf
            gates[g, d] = dot(src[...], wbuf[g]).astype(BF16)

    tr = lax.broadcasted_iota(jnp.int32, (CHUNK, CHUNK), 0)
    tc = lax.broadcasted_iota(jnp.int32, (CHUNK, CHUNK), 1)
    lane = lax.broadcasted_iota(jnp.int32, (CHUNK, LANES), 1)

    def finish(g):
        for d in (0, 1):
            keep = (tr >= tc) if d == 0 else (tr <= tc)
            carry = ents[0][g, d]
            skip = skipw[g][0:1]
            for step in range(count):
                k = step if d == 0 else count - 1 - step
                at = slice(k * CHUNK, (k + 1) * CHUNK)
                ldk = ldg[d, g, at, :]
                since = dot(sin3[d, at], spread[g])
                last = step == count - 1
                carried = dot(proj[d, at, state:], carry.astype(BF16)) * since
                weighted = []
                if not last:
                    to_end = dot(end3[d, at], spread[g])
                for p in range(tiles):
                    part = slice(p * LANES, (p + 1) * LANES)
                    x = inp[g, d, at, part]
                    xf32 = x.astype(F32)
                    mixes = []
                    for h in (2 * p, 2 * p + 1):
                        gap = ldk[:, h : h + 1] - ldt[d, g, h : h + 1, at]
                        gap = jnp.where(keep, gap, 0.0)
                        mix = jnp.where(keep, aff[d, k] * jnp.exp(gap), 0.0)
                        mixes.append((mix * dtt[d, g, h : h + 1, at]).astype(BF16))
                    zero = jnp.zeros_like(x)
                    both = jnp.concatenate(
                        [jnp.where(lane < HEADDIM, x, zero), jnp.where(lane < HEADDIM, zero, x)],
                        axis=0,
                    )
                    out = dot(jnp.concatenate(mixes, axis=1), both)
                    out = out + xf32 * skip[:, part] + carried[:, part]
                    gt = gates[g, d, at, part].astype(F32)
                    out = (out * (gt / (1.0 + jnp.exp(-gt)))).astype(BF16)
                    where = pl.ds(pl.multiple_of(g * cols + p * LANES, LANES), LANES)
                    gated[d, at, where] = out
                    if not last:
                        weighted.append((xf32 * to_end[:, part]).astype(BF16))
                if not last:
                    local = dot_first(proj[d, at, :state], jnp.concatenate(weighted, axis=1))
                    row = CHUNK - 1 if d == 0 else 0
                    carry = carry * since[row : row + 1] + local

    lag = 2 * levels + top - 1
    start = max(2 * groups, lag + 1)

    def slot(s, _):
        @pl.when(s < groups)
        def _():
            states(s)
            up_copy(0, s).start()
            w_copy(gw_ref, s).start()

        @pl.when((s >= groups) & (s < 2 * groups))
        def _():
            gate(s - groups)

        @pl.when(s >= start)
        def _():
            finish(s - start)

        @pl.when(s == 0)
        def _():
            for b in range(total):
                o_copy(b).start()
            for j in range(1, 1 << levels):
                log_copy(j).wait()
            own = logs[0]
            for l in range(levels):
                other = logs[1 << l]
                for j in range((1 << l) + 1, 2 << l):
                    other = other + logs[j]
                coef[2 * l] = jnp.exp(own)
                coef[2 * l + 1] = jnp.exp(other)
                own = own + other
            coef[2 * levels] = jnp.exp(own)

        def stage(off, body):
            g = s - off
            ok = (g >= 0) & (g < groups)

            @pl.when(ok)
            def _():
                body(g)

        for l in range(levels):
            def up(g, l=l):
                up_copy(l, g).wait()
                combine(l, g)
                if l + 1 < levels:
                    up_copy(l + 1, g).start()

            stage(1 + l, up)
        for h in range(top - 1):
            g = s - (levels + h)
            hop(h, g, (g >= 0) & (g < groups))

        def arrive(g):
            for d in (0, 1):
                @pl.when(order(d) == top - 1)
                def _():
                    chain_copy(d, g).wait_recv()

                @pl.when(order(d) < top - 1)
                def _():
                    chain_copy(d, g).wait_send()
            scatter_down(levels - 1, g)
            down_copy(levels - 1, g).start()

        stage(levels + top - 1, arrive)
        for l in range(levels - 1, -1, -1):
            def down(g, l=l):
                down_copy(l, g).wait()
                if l:
                    scatter_down(l - 1, g)
                    down_copy(l - 1, g).start()

            stage(levels + top - 1 + levels - l, down)
        return 0

    lax.fori_loop(0, start + groups, slot, 0)

    for b in range(total):
        o_copy(b).wait()

    def share(b):
        turned = dot(obuf[total - 1 - b], flip).astype(BF16)
        return dot(gated[0], obuf[b]) + dot(gated[1], turned)

    def x_copy(i):
        s = i // per
        return pltpu.make_async_remote_copy(
            src_ref=sbuf.at[i], dst_ref=rbuf.at[i], send_sem=x_send.at[i], recv_sem=x_recv.at[i],
            device_id={"head": lax.rem(side + 1 + s, peers)},
        )

    def give(i, _):
        peer = lax.rem(side + 1 + i // per, peers)
        sbuf[i] = share(peer * per + i % per)
        x_copy(i).start()
        return 0

    lax.fori_loop(0, (peers - 1) * per, give, 0)
    for j in range(per):
        sbuf_own = share(side * per + j)
        for s in range(peers - 1):
            x_copy(s * per + j).wait()
            sbuf_own = sbuf_own + rbuf[s * per + j]
        out_ref[:, j * BLOCK : (j + 1) * BLOCK] = sbuf_own.astype(BF16)


def on_device(
    sequence, input_weight, gate_weight, state_weight, step_weight, step_bias, decay_rate,
    skip_gain, output_weight,
):
    rows, depth = sequence.shape
    width = input_weight.shape[1]
    heads = decay_rate.shape[0]
    state = state_weight.shape[1] // 2
    n = lax.axis_size("seq")
    peers = lax.axis_size("head")
    top = min(n, 4)
    unit = n // top
    levels = unit.bit_length() - 1
    cols = max(LANES, width // 4)
    groups = width // cols
    columns = output_weight.shape[1]
    per = columns // peers // BLOCK
    total = columns // BLOCK
    hg = cols // HEADDIM
    count = rows // CHUNK
    plan = (groups, cols, levels, top, unit, n, peers, heads, per, total)
    moves = (peers - 1) * per
    vmem = pl.BlockSpec(memory_space=pltpu.VMEM)
    hbm = pl.BlockSpec(memory_space=pl.ANY)
    dma = pltpu.SemaphoreType.DMA
    ups = [pltpu.VMEM((groups, 2, state >> l, cols), F32) for l in range(levels + 1)]
    halves = [pltpu.VMEM((groups, 2, state >> (l + 1), cols), F32) for l in range(levels)]
    ents = [pltpu.VMEM((groups, 2, state >> l, cols), F32) for l in range(levels)]
    chain = pltpu.VMEM((groups, 2, state >> levels, cols), F32)
    return pl.pallas_call(
        functools.partial(layer_kernel, plan),
        in_specs=[vmem] * 6 + [hbm] * 3,
        out_specs=vmem,
        out_shape=jax.ShapeDtypeStruct((rows, columns // peers), BF16),
        scratch_shapes=[
            pltpu.VMEM((rows, depth), BF16),
            pltpu.VMEM((2, rows, 2 * state), BF16),
            pltpu.VMEM((2, groups, rows, LANES), F32),
            pltpu.VMEM((2, groups, hg, rows), F32),
            pltpu.VMEM((2, groups, hg, rows), F32),
            pltpu.VMEM((2, rows, LANES), BF16),
            pltpu.VMEM((2, rows, LANES), BF16),
            pltpu.VMEM((2, rows, LANES), BF16),
            pltpu.VMEM((groups, LANES, cols), BF16),
            pltpu.VMEM((2, count, CHUNK, CHUNK), F32),
            pltpu.VMEM((groups, 8, cols), F32),
            pltpu.VMEM((1 << levels, 2, groups, STEP, LANES), F32),
            pltpu.VMEM((2 * levels + 1, 2, groups, STEP, LANES), F32),
            pltpu.VMEM((groups, depth, cols), BF16),
            pltpu.VMEM((total, width, BLOCK), BF16),
            pltpu.VMEM((groups, 2, rows, cols), BF16),
            pltpu.VMEM((groups, 2, rows, cols), BF16),
            pltpu.VMEM((2, rows, width), BF16),
            ups,
            halves,
            chain,
            chain,
            ents,
            halves,
            pltpu.VMEM((moves, rows, BLOCK), F32),
            pltpu.VMEM((moves, rows, BLOCK), F32),
            dma((groups,)),
            dma((total,)),
            dma((1 << levels,)),
            dma((1 << levels,)),
            dma((levels, groups)),
            dma((levels, groups)),
            dma((2, groups)),
            dma((2, groups)),
            dma((levels, groups)),
            dma((levels, groups)),
            dma((moves,)),
            dma((moves,)),
        ],
        compiler_params=pltpu.CompilerParams(
            collective_id=0, has_side_effects=True, vmem_limit_bytes=66_000_000
        ),
    )(
        sequence, state_weight, step_weight, step_bias.reshape(1, heads),
        decay_rate.reshape(1, heads), skip_gain.reshape(1, heads), input_weight, gate_weight,
        output_weight,
    )


def solution(mesh):
    placed = (
        P("seq", None),
        P(None, "head"),
        P(None, "head"),
        P(),
        P(None, "head"),
        P("head"),
        P("head"),
        P("head"),
        P("head", None),
    )
    return jax.shard_map(
        on_device, mesh=mesh, in_specs=placed, out_specs=P("seq", "head"), check_vma=False
    )
```

```python
import functools

import jax
import jax.numpy as jnp
from jax import lax
from jax.experimental import pallas as pl
from jax.experimental.pallas import tpu as pltpu
from jax.sharding import PartitionSpec as P

F32 = jnp.float32
BF16 = jnp.bfloat16
HEADDIM = 64
CHUNK = 128
LANES = 128
BLOCK = 256
GROUPS = 4
FAR = 3
HOP = 2


def eye_flip(size):
    r = lax.broadcasted_iota(jnp.int32, (size, size), 0)
    c = lax.broadcasted_iota(jnp.int32, (size, size), 1)
    return jnp.where(r + c == size - 1, 1.0, 0.0).astype(BF16)


def dot(a, b):
    return jnp.dot(a, b, preferred_element_type=F32)


def dot_last(a, b):
    return lax.dot_general(a, b, (((1,), (1,)), ((), ())), preferred_element_type=F32)


def split(a):
    hi = a.astype(BF16)
    rest = a - hi.astype(F32)
    mid = rest.astype(BF16)
    low = (rest - mid.astype(F32)).astype(BF16)
    return hi, mid, low


def split_lanes(a, heads):
    hi, mid, low = split(a)
    lane = lax.broadcasted_iota(jnp.int32, a.shape, 1)
    low = jnp.where(lane < 3 * heads, low.astype(F32), 0.0)
    return jnp.where(
        lane < heads, hi.astype(F32), jnp.where(lane < 2 * heads, mid.astype(F32), low)
    ).astype(BF16)


def repeat_of(heads, turned=False):
    shape = (LANES, heads) if turned else (heads, LANES)
    r = lax.broadcasted_iota(jnp.int32, shape, 1 if turned else 0)
    c = lax.broadcasted_iota(jnp.int32, shape, 0 if turned else 1)
    hit = (c == r) | (c == r + heads) | (c == r + 2 * heads)
    return jnp.where(hit, 1.0, 0.0).astype(BF16)


def spread_of(heads, first, cols):
    r = lax.broadcasted_iota(jnp.int32, (LANES, cols), 0)
    c = lax.broadcasted_iota(jnp.int32, (LANES, cols), 1)
    head = lax.shift_right_logical(c, 6) + first
    hit = (r == head) | (r == head + heads) | (r == head + 2 * heads)
    return jnp.where(hit, 1.0, 0.0).astype(BF16)


def layer_kernel(
    plan,
    sw_ref, bias_ref, rate_ref, gain_ref, x_hbm, stw_hbm, inw_ref, gw_ref, ow_ref,
    out_ref,
    x_ref, stw_ref, xf, ldv, stv, proj, turned_b, ldg, ldt, dtt, fac3, sin3, end3, spread, aff, skipw, logs, coef,
    wbuf, obuf, inp, gates, gated,
    ups, gots, chin, chout, ents, outs, sbuf, rbuf,
    in_sem, w_sem, o_sem, lg_send, lg_recv, up_send, up_recv, ch_send, ch_recv, dn_send, dn_recv,
    x_send, x_recv,
):
    (groups, cols, levels, top, unit, n, peers, heads, per, total) = plan
    rows, depth = x_ref.shape
    state = stw_ref.shape[1] // 2
    hg = cols // HEADDIM
    tiles = cols // LANES
    count = rows // CHUNK
    me = lax.axis_index("seq")
    side = lax.axis_index("head")
    pos = me // unit
    bits = [(me // (1 << l)) % 2 for l in range(levels)]

    def mate(j):
        at = me
        for l in range(levels):
            if (j >> l) & 1:
                at = at + (1 << l) * (1 - 2 * bits[l])
        return at

    def ring(step):
        return me + (lax.rem(pos + step + top, top) - pos) * unit

    def w_copy(src, g):
        return pltpu.make_async_copy(
            src.at[:, pl.ds(pl.multiple_of(g * cols, LANES), cols)], wbuf.at[g], w_sem.at[g]
        )

    def o_copy(b):
        return pltpu.make_async_copy(
            ow_ref.at[:, pl.ds(b * BLOCK, BLOCK)], obuf.at[b], o_sem.at[b]
        )

    x_in = pltpu.make_async_copy(x_hbm, x_ref, in_sem.at[0])
    stw_in = pltpu.make_async_copy(stw_hbm, stw_ref, in_sem.at[1])
    x_in.start()
    stw_in.start()
    for g in range(groups):
        w_copy(inw_ref, g).start()

    barrier = pltpu.get_barrier_semaphore()
    greet = [mate(j) for j in range(1, 1 << levels)] + [ring(1), ring(-1)]
    for who in greet:
        pl.semaphore_signal(barrier, inc=1, device_id={"seq": who})
    for s in range(1, peers):
        pl.semaphore_signal(barrier, inc=1, device_id={"head": lax.rem(side + s, peers)})
    for d in (0, 1):
        @pl.when((pos if d == 0 else top - 1 - pos) == 0)
        def _():
            chin[:, d] = jnp.zeros_like(chin[:, d])
    rep = repeat_of(heads)
    sw3 = dot(repeat_of(heads, True), sw_ref[...]).astype(BF16)

    def tripled(ref):
        wide = jnp.broadcast_to(ref[...], (8, heads))
        a, b, c = split(wide)
        return dot(a, rep) + dot(b, rep) + dot(c, rep)

    bias = tripled(bias_ref)[0:1]
    rate = tripled(rate_ref)[0:1]
    for g in range(groups):
        spread[g] = spread_of(heads, g * hg, cols)
    flip = eye_flip(BLOCK)
    blocks = depth // BLOCK
    x_in.wait()
    for b in range(blocks):
        xf[:, b * BLOCK : (b + 1) * BLOCK] = dot(
            x_ref[:, (blocks - 1 - b) * BLOCK : (blocks - b) * BLOCK], flip
        ).astype(BF16)
    r = lax.broadcasted_iota(jnp.int32, (rows, rows), 0)
    c = lax.broadcasted_iota(jnp.int32, (rows, rows), 1)
    for d in (0, 1):
        src = x_ref if d == 0 else xf
        raw = dot_last(src[...], sw3) + bias
        soft = jnp.maximum(raw, 0.0) + jnp.log1p(jnp.exp(-jnp.abs(raw)))
        steps = soft.astype(BF16).astype(F32)
        tri = jnp.where((r >= c) if d == 0 else (r <= c), 1.0, 0.0).astype(BF16)
        va, vb, vc = split(-rate * steps)
        ld = dot(tri, va) + dot(tri, vb) + dot(tri, vc)
        end = ld[rows - 1 : rows] if d == 0 else ld[0:1]
        fac3[d] = split_lanes(jnp.exp(end - ld) * steps, heads)
        ldv[d] = ld
        stv[d] = steps
        ends = split_lanes(jnp.broadcast_to(end, (8, LANES)), heads)
        for g in range(groups):
            wide = dot(ends, spread[g])
            for j in range(tiles):
                row = g * tiles + j
                logs[0, d, row : row + 1] = wide[0:1, j * LANES : (j + 1) * LANES]
    stw_in.wait()
    for d in (0, 1):
        src = x_ref if d == 0 else xf
        both = dot(src[...], stw_ref[...])
        proj[d] = both.astype(BF16)
        turned_b[d] = both[:, :state].T.astype(BF16)
    pl.semaphore_wait(barrier, len(greet) + peers - 1)

    def tables(d):
        ld = ldv[d]
        steps = stv[d]
        for k in range(count):
            at = slice(k * CHUNK, (k + 1) * CHUNK)
            ldk = ld[at]
            if d == 0:
                edge = ld[(k + 1) * CHUNK - 1 : (k + 1) * CHUNK]
                prev = ld[k * CHUNK - 1 : k * CHUNK] if k else None
            else:
                edge = ld[k * CHUNK : k * CHUNK + 1]
                prev = ld[(k + 1) * CHUNK : (k + 1) * CHUNK + 1] if k < count - 1 else None
            sin3[d, at] = split_lanes(jnp.exp(ldk if prev is None else ldk - prev), heads)
            end3[d, at] = split_lanes(jnp.exp(edge - ldk) * steps[at], heads)
            aff[d, k] = dot(proj[d, at, state:], turned_b[d, :, at])
        flat_ld = ld.T
        flat_dt = steps.T
        for g in range(groups):
            ldg[d, g] = pltpu.roll(ld, LANES - g * hg, axis=1) if g else ld
            ldt[d, g] = flat_ld[g * hg : (g + 1) * hg]
            dtt[d, g] = flat_dt[g * hg : (g + 1) * hg]

    def skips():
        gain = split_lanes(tripled(gain_ref), heads)
        for g in range(groups):
            skipw[g] = dot(gain, spread[g])

    def log_copy(j):
        return pltpu.make_async_remote_copy(
            src_ref=logs.at[0], dst_ref=logs.at[j], send_sem=lg_send.at[j],
            recv_sem=lg_recv.at[j], device_id={"seq": mate(j)},
        )

    def half_of(l):
        return state >> (l + 1)

    def rows_at(l, flag):
        return pl.ds(pl.multiple_of(flag * half_of(l), 8), half_of(l))

    def up_copy(l, g):
        return pltpu.make_async_remote_copy(
            src_ref=ups[l].at[g, :, rows_at(l, 1 - bits[l]), :], dst_ref=gots[l].at[g],
            send_sem=up_send.at[l, g], recv_sem=up_recv.at[l, g],
            device_id={"seq": mate(1 << l)},
        )

    def chain_copy(d, g):
        return pltpu.make_async_remote_copy(
            src_ref=chout.at[g, d], dst_ref=chin.at[g, d], send_sem=ch_send.at[d, g],
            recv_sem=ch_recv.at[d, g], device_id={"seq": ring(1 if d == 0 else -1)},
        )

    def down_copy(l, g):
        return pltpu.make_async_remote_copy(
            src_ref=outs[l].at[g], dst_ref=ents[l].at[g, :, rows_at(l, bits[l]), :],
            send_sem=dn_send.at[l, g], recv_sem=dn_recv.at[l, g],
            device_id={"seq": mate(1 << l)},
        )

    def late(l, d):
        flag = bits[l] if d == 0 else 1 - bits[l]
        return flag.astype(F32)

    def own_coef(l, d, g, j):
        return coef[2 * l, d, pl.ds(g * tiles + j, 1), :]

    def other_coef(l, d, g, j):
        return coef[2 * l + 1, d, pl.ds(g * tiles + j, 1), :]

    def combine(l, g):
        mine = rows_at(l, bits[l])
        for d in (0, 1):
            f = late(l, d)
            for j in range(tiles):
                ea = f + (1.0 - f) * other_coef(l, d, g, j)
                eb = (1.0 - f) + f * own_coef(l, d, g, j)
                at = slice(j * LANES, (j + 1) * LANES)
                ups[l + 1][g, d, :, at] = (
                    ea * ups[l][g, d, mine, at] + eb * gots[l][g, d, :, at]
                )

    def scatter_down(l, g):
        mine = rows_at(l, bits[l])
        for d in (0, 1):
            f = late(l, d)
            for j in range(tiles):
                keep = f * other_coef(l, d, g, j) + (1.0 - f)
                give = f + (1.0 - f) * own_coef(l, d, g, j)
                at = slice(j * LANES, (j + 1) * LANES)
                enter = chin[g, d, :, at] if l == levels - 1 else ents[l + 1][g, d, :, at]
                outs[l][g, d, :, at] = (
                    give * enter + (1.0 - f) * ups[l][g, d, mine, at]
                )
                ents[l][g, d, mine, at] = keep * enter + f * gots[l][g, d, :, at]

    def order(d):
        return pos if d == 0 else top - 1 - pos

    def hop(h, g):
        for d in (0, 1):
            @pl.when(order(d) == h)
            def _():
                if h:
                    chain_copy(d, g).wait_recv()
                for j in range(tiles):
                    at = slice(j * LANES, (j + 1) * LANES)
                    whole = coef[2 * levels, d, pl.ds(g * tiles + j, 1), :]
                    chout[g, d, :, at] = (
                        whole * chin[g, d, :, at] + ups[levels][g, d, :, at]
                    )
                chain_copy(d, g).start()

    for j in range(1, 1 << levels):
        log_copy(j).start()

    def states(g, d):
        if d == 0:
            w_copy(inw_ref, g).wait()
        src = x_ref if d == 0 else xf
        x = dot(src[...], wbuf[g]).astype(BF16)
        inp[g, d] = x
        wide = dot(fac3[d], spread[g])
        weighted = (inp[g, d].astype(F32) * wide).astype(BF16)
        ups[0][g, d] = dot(turned_b[d], weighted)

    def gate(g, d):
        if d == 0:
            w_copy(gw_ref, g).wait()
        src = x_ref if d == 0 else xf
        gates[g, d] = dot(src[...], wbuf[g]).astype(BF16)

    tr = lax.broadcasted_iota(jnp.int32, (CHUNK, CHUNK), 0)
    tc = lax.broadcasted_iota(jnp.int32, (CHUNK, CHUNK), 1)
    lane = lax.broadcasted_iota(jnp.int32, (CHUNK, LANES), 1)

    def finish(g, d):
        keep = (tr >= tc) if d == 0 else (tr <= tc)
        carry = ents[0][g, d]
        skip = skipw[g][0:1]
        for step in range(count):
            k = step if d == 0 else count - 1 - step
            at = slice(k * CHUNK, (k + 1) * CHUNK)
            ldk = ldg[d, g, at, :]
            since = dot(sin3[d, at], spread[g])
            last = step == count - 1
            carried = dot(proj[d, at, state:], carry.astype(BF16)) * since
            weighted = []
            if not last:
                to_end = dot(end3[d, at], spread[g])
            for p in range(tiles):
                part = slice(p * LANES, (p + 1) * LANES)
                x = inp[g, d, at, part]
                xf32 = x.astype(F32)
                mixes = []
                for h in (2 * p, 2 * p + 1):
                    gap = ldk[:, h : h + 1] - ldt[d, g, h : h + 1, at]
                    gap = jnp.where(keep, gap, 0.0)
                    mix = jnp.where(keep, aff[d, k] * jnp.exp(gap), 0.0)
                    mixes.append((mix * dtt[d, g, h : h + 1, at]).astype(BF16))
                zero = jnp.zeros_like(x)
                both = jnp.concatenate(
                    [jnp.where(lane < HEADDIM, x, zero), jnp.where(lane < HEADDIM, zero, x)],
                    axis=0,
                )
                out = dot(jnp.concatenate(mixes, axis=1), both)
                out = out + xf32 * skip[:, part] + carried[:, part]
                gt = gates[g, d, at, part].astype(F32)
                out = (out * (gt / (1.0 + jnp.exp(-gt)))).astype(BF16)
                where = pl.ds(pl.multiple_of(g * cols + p * LANES, LANES), LANES)
                gated[d, at, where] = out
                if not last:
                    weighted.append((xf32 * to_end[:, part]).astype(BF16))
            if not last:
                local = dot(turned_b[d, :, at], jnp.concatenate(weighted, axis=1))
                row = CHUNK - 1 if d == 0 else 0
                carry = carry * since[row : row + 1] + local

    lat = [1] + [FAR] * (levels - 1)
    up_at = [sum(lat[: l + 1]) for l in range(levels)]
    hop_at = [up_at[-1] + HOP * h for h in range(top)]
    down_at = [hop_at[-1] + sum(lat[l:]) for l in range(levels)]
    lag = down_at[0]
    start = max(groups + 1, lag // 2 + 1)

    def half_slot(i, half):
        def during(first, body, length=groups):
            @pl.when((i >= first) & (i < first + length))
            def _():
                body(i - first)

        def open_group(g):
            states(g, half)
            if half:
                up_copy(0, g).start()
                w_copy(gw_ref, g).start()

        during(0, open_group)
        during(groups, lambda g: gate(g, half))
        during(groups, lambda _: tables(half), 1)
        if half:
            during(groups + 1, lambda _: skips(), 1)
        during(start, lambda g: finish(g, half))

        def first(_):
            for b in range(total):
                o_copy(b).start()
            for j in range(1, 1 << levels):
                log_copy(j).wait()
            own = logs[0]
            for l in range(levels):
                other = logs[1 << l]
                for j in range((1 << l) + 1, 2 << l):
                    other = other + logs[j]
                coef[2 * l] = jnp.exp(own)
                coef[2 * l + 1] = jnp.exp(other)
                own = own + other
            coef[2 * levels] = jnp.exp(own)

        if half == 0:
            during(1, first, 1)

        def stage(off, body):
            if (1 + off - half) % 2 == 0:
                during((1 + off - half) // 2, body)

        for l in range(levels):
            def up(g, l=l):
                up_copy(l, g).wait()
                combine(l, g)
                if l + 1 < levels:
                    up_copy(l + 1, g).start()

            stage(up_at[l], up)
        for h in range(top - 1):
            stage(hop_at[h], lambda g, h=h: hop(h, g))

        def arrive(g):
            for d in (0, 1):
                @pl.when(order(d) == top - 1)
                def _():
                    chain_copy(d, g).wait_recv()

                @pl.when(order(d) < top - 1)
                def _():
                    chain_copy(d, g).wait_send()
            scatter_down(levels - 1, g)
            down_copy(levels - 1, g).start()

        stage(hop_at[-1], arrive)
        for l in range(levels - 1, -1, -1):
            def down(g, l=l):
                down_copy(l, g).wait()
                if l:
                    scatter_down(l - 1, g)
                    down_copy(l - 1, g).start()

            stage(down_at[l], down)

    def slot(i, _):
        half_slot(i, 0)
        half_slot(i, 1)
        return 0

    lax.fori_loop(0, start + groups, slot, 0)

    for b in range(total):
        o_copy(b).wait()

    def share(b):
        turned = dot(obuf[total - 1 - b], flip).astype(BF16)
        return dot(gated[0], obuf[b]) + dot(gated[1], turned)

    def x_copy(i):
        s = i // per
        return pltpu.make_async_remote_copy(
            src_ref=sbuf.at[i], dst_ref=rbuf.at[i], send_sem=x_send.at[i], recv_sem=x_recv.at[i],
            device_id={"head": lax.rem(side + 1 + s, peers)},
        )

    def give(i, _):
        peer = lax.rem(side + 1 + i // per, peers)
        sbuf[i] = share(peer * per + i % per)
        x_copy(i).start()
        return 0

    lax.fori_loop(0, (peers - 1) * per, give, 0)
    for j in range(per):
        sbuf_own = share(side * per + j)
        for s in range(peers - 1):
            x_copy(s * per + j).wait()
            sbuf_own = sbuf_own + rbuf[s * per + j]
        out_ref[:, j * BLOCK : (j + 1) * BLOCK] = sbuf_own.astype(BF16)


def on_device(
    sequence, input_weight, gate_weight, state_weight, step_weight, step_bias, decay_rate,
    skip_gain, output_weight,
):
    rows, depth = sequence.shape
    width = input_weight.shape[1]
    heads = decay_rate.shape[0]
    state = state_weight.shape[1] // 2
    n = lax.axis_size("seq")
    peers = lax.axis_size("head")
    top = min(n, 4)
    unit = n // top
    levels = unit.bit_length() - 1
    cols = max(LANES, width // GROUPS)
    groups = width // cols
    columns = output_weight.shape[1]
    per = columns // peers // BLOCK
    total = columns // BLOCK
    hg = cols // HEADDIM
    count = rows // CHUNK
    plan = (groups, cols, levels, top, unit, n, peers, heads, per, total)
    moves = (peers - 1) * per
    vmem = pl.BlockSpec(memory_space=pltpu.VMEM)
    hbm = pl.BlockSpec(memory_space=pl.ANY)
    dma = pltpu.SemaphoreType.DMA
    ups = [pltpu.VMEM((groups, 2, state >> l, cols), F32) for l in range(levels + 1)]
    halves = [pltpu.VMEM((groups, 2, state >> (l + 1), cols), F32) for l in range(levels)]
    ents = [pltpu.VMEM((groups, 2, state >> l, cols), F32) for l in range(levels)]
    chain = pltpu.VMEM((groups, 2, state >> levels, cols), F32)
    return pl.pallas_call(
        functools.partial(layer_kernel, plan),
        in_specs=[vmem] * 4 + [hbm] * 5,
        out_specs=vmem,
        out_shape=jax.ShapeDtypeStruct((rows, columns // peers), BF16),
        scratch_shapes=[
            pltpu.VMEM((rows, depth), BF16),
            pltpu.VMEM((depth, 2 * state), BF16),
            pltpu.VMEM((rows, depth), BF16),
            pltpu.VMEM((2, rows, LANES), F32),
            pltpu.VMEM((2, rows, LANES), F32),
            pltpu.VMEM((2, rows, 2 * state), BF16),
            pltpu.VMEM((2, state, rows), BF16),
            pltpu.VMEM((2, groups, rows, LANES), F32),
            pltpu.VMEM((2, groups, hg, rows), F32),
            pltpu.VMEM((2, groups, hg, rows), F32),
            pltpu.VMEM((2, rows, LANES), BF16),
            pltpu.VMEM((2, rows, LANES), BF16),
            pltpu.VMEM((2, rows, LANES), BF16),
            pltpu.VMEM((groups, LANES, cols), BF16),
            pltpu.VMEM((2, count, CHUNK, CHUNK), F32),
            pltpu.VMEM((groups, 8, cols), F32),
            pltpu.VMEM((1 << levels, 2, width // LANES, LANES), F32),
            pltpu.VMEM((2 * levels + 1, 2, width // LANES, LANES), F32),
            pltpu.VMEM((groups, depth, cols), BF16),
            pltpu.VMEM((total, width, BLOCK), BF16),
            pltpu.VMEM((groups, 2, rows, cols), BF16),
            pltpu.VMEM((groups, 2, rows, cols), BF16),
            pltpu.VMEM((2, rows, width), BF16),
            ups,
            halves,
            chain,
            chain,
            ents,
            halves,
            pltpu.VMEM((moves, rows, BLOCK), F32),
            pltpu.VMEM((moves, rows, BLOCK), F32),
            dma((2,)),
            dma((groups,)),
            dma((total,)),
            dma((1 << levels,)),
            dma((1 << levels,)),
            dma((levels, groups)),
            dma((levels, groups)),
            dma((2, groups)),
            dma((2, groups)),
            dma((levels, groups)),
            dma((levels, groups)),
            dma((moves,)),
            dma((moves,)),
        ],
        compiler_params=pltpu.CompilerParams(
            collective_id=0, has_side_effects=True, vmem_limit_bytes=66_000_000
        ),
    )(
        step_weight.T, step_bias.reshape(1, heads), decay_rate.reshape(1, heads),
        skip_gain.reshape(1, heads), sequence, state_weight, input_weight, gate_weight,
        output_weight,
    )


def solution(mesh):
    placed = (
        P("seq", None),
        P(None, "head"),
        P(None, "head"),
        P(),
        P(None, "head"),
        P("head"),
        P("head"),
        P("head"),
        P("head", None),
    )
    return jax.shard_map(
        on_device, mesh=mesh, in_specs=placed, out_specs=P("seq", "head"), check_vma=False
    )
```
